32 devices in a mesh: section: 4 (over y, core), mp: 8 (over z, x).
Axes of the slice: x: 2, y: 2, z: 4, core: 2. Of those that a mesh axis runs over, the one named last changes fastest.
Arguments:
- arriving: bfloat16 [4, 768, 8192], P('section', None, 'mp'), may hold values from -6 to 6
- norm_gain: bfloat16 [4, 8192], P('section'), may hold values from 0.099609375 to 1.8984375
- w_query: bfloat16 [4, 2048, 8192], P('section', 'mp'), may hold values from -26 to 26
- w_key: bfloat16 [4, 1024, 8192], P('section', 'mp'), may hold values from -1 to 1
- w_value: bfloat16 [4, 1024, 8192], P('section', 'mp'), may hold values from -0.25 to 0.25
- w_out: bfloat16 [4, 2048, 8192], P('section', 'mp'), may hold values from -0.125 to 0.125
Outputs:
- attended: bfloat16 [4, 768, 8192], P('section', 'mp')
- stream_next: bfloat16 [4, 768, 8192], P('section', 'mp')
The draws below stay inside these ranges and needn't reach their ends.
All inputs are finite; a program needn't handle non-finite values.
Results may differ from the reference program's by a relative error of at most 0.017.
Values may be sent and summed in bfloat16 or wider, within the bound.
A program may use at most 128 MiB of HBM per device.

```python
import math
import jax
import jax.numpy as jnp
from jax import lax

D = 8192
HD = 128
KV_HEADS = 8
HQ_DEV = 2
HEADS = 16
KVD = 1024
LENGTH = 768
SECTIONS = 4


def key_rows(key):
    fresh = jax.random.normal(jax.random.fold_in(key, 11), (SECTIONS, KVD, D), jnp.float32)
    return jnp.clip(fresh, -5.0, 5.0) / math.sqrt(D)


def draw_w_key(key, part):
    return key_rows(key).astype(jnp.bfloat16)


def draw_w_query(key, part):
    fresh = jax.random.normal(jax.random.fold_in(key, 23), (SECTIONS, HEADS * HD, D), jnp.float32)
    fresh = jnp.clip(fresh, -5.0, 5.0) / math.sqrt(D)
    return fresh.astype(jnp.bfloat16)


def shard_levels(own_key, shape, cuts, low, largest):
    level = 1.0
    for position, shards_of in cuts:
        draws = jax.random.uniform(jax.random.fold_in(jax.random.fold_in(own_key, 6), position), (shards_of,), jnp.float32, low / len(cuts), largest / len(cuts))
        level = level * jnp.repeat(jnp.exp(draws), shape[position] // shards_of).reshape((-1,) + (1,) * (len(shape) - 1 - position))
    return level


def gaussian(stream_key, shape, scale, most, split=(), held_as=jnp.bfloat16):
    drawn = scale * jax.random.normal(stream_key, shape, jnp.float32)
    if split:
        drawn = drawn * shard_levels(stream_key, shape, split, -0.22, 0.18)
    return jnp.clip(drawn, -most, most).astype(held_as)


def setup_inputs(seed: int = 0) -> dict:
    splits = jax.random.split(jax.random.key(seed), 7)
    return {
        "arriving": gaussian(splits[0], (SECTIONS, LENGTH, D), 1.0, 6.0, ((0, 4), (2, 8))),
        "norm_gain": jnp.clip(1.0 + 0.18 * jax.random.normal(splits[1], (SECTIONS, D), jnp.float32), 0.099609375, 1.8984375).astype(jnp.bfloat16),
        "w_query": draw_w_query(jax.random.fold_in(splits[6], 71), 0),
        "w_key": draw_w_key(jax.random.fold_in(splits[6], 71), 0),
        "w_value": gaussian(splits[4], (SECTIONS, KVD, D), (D // 16) ** -0.5, 0.25, ((0, 4), (1, 8))),
        "w_out": gaussian(splits[5], (SECTIONS, HEADS * HD, D), (HEADS * HD) ** -0.5, 0.125, ((0, 4), (1, 8))),
    }


rope_base = 500000.0
norm_eps = 1e-05

def rotate(channel_major, first_channel):
    channels = channel_major.shape[0]
    length = channel_major.shape[1]
    within = (jnp.arange(channels, dtype=jnp.int32) + first_channel) % HD
    pair_index = (within // 2).astype(channel_major.dtype)
    frequency = jnp.exp(pair_index * (-2.0 * math.log(rope_base) / HD))
    positions = jnp.arange(length, dtype=jnp.int32).astype(channel_major.dtype)
    angles = frequency[0::2, None] * positions[None, :]
    cos_table = jnp.cos(angles)
    sine_table = jnp.sin(angles)
    paired = channel_major.reshape(channels // 2, 2, length)
    even_part = paired[:, 0]
    odd_part = paired[:, 1]
    rotated = jnp.stack([even_part * cos_table - odd_part * sine_table, even_part * sine_table + odd_part * cos_table], axis=1)
    return rotated.reshape(channels, length)

def head_order(pair_major):
    length = pair_major.shape[1]
    grouped = pair_major.reshape(HD // 2, KV_HEADS, 2, length)
    return jnp.transpose(grouped, (1, 0, 2, 3)).reshape(KV_HEADS * HD, length)

def normalize(hidden_in, gain_row):
    as_float = hidden_in.astype(jnp.float32)
    mean_square = lax.optimization_barrier(jnp.mean(as_float * as_float, axis=1, keepdims=True))
    normed = (as_float * lax.rsqrt(mean_square + norm_eps) * gain_row.astype(jnp.float32)).astype(jnp.bfloat16)
    return (as_float, normed)

def reference(arriving, norm_gain, w_query, w_key, w_value, w_out):
    group_size = HEADS // KV_HEADS
    width = HQ_DEV * HD
    score_scale = 1.0 / math.sqrt(HD)
    attended_all = []
    stream_all = []
    for section in range(SECTIONS):
        as_float, normed = normalize(arriving[(section - 1) % SECTIONS], norm_gain[section])
        length = normed.shape[0]
        queries = rotate(jnp.dot(w_query[section], normed.T, preferred_element_type=jnp.float32), 0).astype(jnp.bfloat16)
        key_all = rotate(head_order(jnp.dot(w_key[section], normed.T, preferred_element_type=jnp.float32)), 0).astype(jnp.bfloat16)
        value_all = head_order(jnp.dot(w_value[section], normed.T, preferred_element_type=jnp.float32)).astype(jnp.bfloat16)
        query_heads = queries.reshape(HEADS, HD, length).astype(jnp.float32)
        key_heads = jnp.repeat(key_all.reshape(KV_HEADS, HD, length), group_size, axis=0).astype(jnp.float32)
        value_heads = jnp.repeat(value_all.reshape(KV_HEADS, HD, length), group_size, axis=0).astype(jnp.float32)
        scores = jnp.einsum('hdi,hdj->hij', query_heads, key_heads) * score_scale
        token_index = jnp.arange(length, dtype=jnp.int32)
        causal = token_index[:, None] >= token_index[None, :]
        scores = jnp.where(causal[None], scores, -1e+30)
        row_max = lax.optimization_barrier(jnp.max(scores, axis=-1, keepdims=True))
        exponent = jnp.exp(scores - row_max)
        row_total = lax.optimization_barrier(jnp.sum(exponent, axis=-1, keepdims=True))
        weights = (exponent / row_total).astype(jnp.bfloat16)
        context = jnp.einsum('hij,hdj->ihd', weights.astype(jnp.float32), value_heads).astype(jnp.bfloat16)
        context = context.reshape(length, HEADS * HD)
        summed = jnp.zeros((length, D), jnp.float32)
        for shard in range(HEADS // HQ_DEV):
            partial_term = jnp.dot(context[:, shard * width:(shard + 1) * width], w_out[section][shard * width:(shard + 1) * width], preferred_element_type=jnp.float32)
            summed = summed + lax.optimization_barrier(partial_term.astype(jnp.bfloat16)).astype(jnp.float32)
        attended_all.append(summed.astype(jnp.bfloat16))
        stream_all.append((as_float + summed).astype(jnp.bfloat16))
    return (jnp.stack(attended_all), jnp.stack(stream_all))
```

```python
import functools
import math

import jax
import jax.numpy as jnp
import numpy as np
from jax import lax
from jax.experimental import pallas as pl
from jax.experimental.pallas import tpu as pltpu
from jax.sharding import PartitionSpec as P

HD = 128
KV_HEADS = 8
ROPE_BASE = 500000.0
NORM_EPS = 1e-05
MESH = pl.DeviceIdType.MESH
VMEM_LIMIT = 64000000


def ring_position(member, n):
    return jnp.where(member % 2 == 0, member // 2, n - 1 - member // 2)


def ring_member(position, n):
    position = lax.rem(position + 2 * n, n)
    return jnp.where(position < n // 2, 2 * position, 2 * (n - 1 - position) + 1)


def swap_pairs(x):
    lane = lax.broadcasted_iota(jnp.int32, x.shape, 1)
    width = x.shape[1]
    return jnp.where(lane % 2 == 0, pltpu.roll(x, width - 1, 1), pltpu.roll(x, 1, 1))


def gather_kernel(
    n, chunks, arriving, gain, wq, wk, wv, cos_ref, sin_ref,
    q_out, k_out, v_out, resid_out,
    x_all, weights, acc, squares, w_sem, shift_send, shift_recv, ring_send, ring_recv,
):
    sections = lax.axis_size("section")
    section = lax.axis_index("section")
    me = lax.axis_index("mp")
    position = ring_position(me, n)
    right, left = ring_member(position + 1, n), ring_member(position - 1, n)
    following, previous = lax.rem(section + 1, sections), lax.rem(section + sections - 1, sections)
    hops = n // 2
    per = n // chunks
    rows = x_all.shape[2]
    width = x_all.shape[3]
    chunk_rows = per * rows
    qw, kw, vw = wq.shape[0], wk.shape[0], wv.shape[0]

    def weight_copy(j, part):
        src, start, size = ((wq, 0, qw), (wk, qw, kw), (wv, qw + kw, vw))[part]
        return pltpu.make_async_copy(
            src.at[:, pl.ds(j * width, width)], weights.at[j, pl.ds(start, size)], w_sem.at[j, part]
        )

    barrier = pltpu.get_barrier_semaphore()
    for partner in (right, left):
        pl.semaphore_signal(barrier, inc=1, device_id={"mp": partner}, device_id_type=MESH)
    for partner in (following, previous):
        pl.semaphore_signal(barrier, inc=1, device_id={"section": partner}, device_id_type=MESH)
    pl.semaphore_wait(barrier, 4)

    def shift_copy(c):
        return pltpu.make_async_remote_copy(
            src_ref=arriving.at[pl.ds(c * per, per)],
            dst_ref=x_all.at[me, pl.ds(c * per, per)],
            send_sem=shift_send.at[c], recv_sem=shift_recv.at[c],
            device_id={"section": following}, device_id_type=MESH,
        )

    def ring_copy(way, hop, c):
        origin = ring_member(position - (hop - 1) if way == 0 else position + (hop - 1), n)
        return pltpu.make_async_remote_copy(
            src_ref=x_all.at[origin, pl.ds(c * per, per)],
            dst_ref=x_all.at[origin, pl.ds(c * per, per)],
            send_sem=ring_send.at[way, hop - 1, c], recv_sem=ring_recv.at[way, hop - 1, c],
            device_id={"mp": right if way == 0 else left}, device_id_type=MESH,
        )

    for c in range(chunks):
        shift_copy(c).start()
    for j in range(n):
        for part in range(3):
            weight_copy(j, part).start()
    acc[...] = jnp.zeros_like(acc)
    squares[...] = jnp.zeros_like(squares)

    def compute(slot, c):
        x = x_all[slot, pl.ds(c * per, per)].astype(jnp.float32).reshape(chunk_rows, width)
        total = x[:, :128] * x[:, :128]
        for g in range(1, width // 128):
            part = x[:, g * 128 : (g + 1) * 128]
            total = total + part * part
        squares[c] += total
        scaled = (x * gain[slot]).astype(jnp.bfloat16)
        acc[c] += lax.dot_general(
            scaled, weights[slot], (((1,), (1,)), ((), ())), preferred_element_type=jnp.float32
        )

    for c in range(chunks):
        shift_copy(c).wait_recv()
        ring_copy(0, 1, c).start()
        ring_copy(1, 1, c).start()
    for j in range(n):
        for part in range(3):
            weight_copy(j, part).wait()

    @pl.loop(0, chunks)
    def _(c):
        compute(me, c)

    @pl.loop(0, hops * chunks)
    def _(i):
        hop = i // chunks + 1
        c = lax.rem(i, chunks)
        last = hop == hops
        low = c < chunks // 2
        for way in range(2):
            mine = low if way == 0 else jnp.logical_not(low)
            origin = ring_member(position - hop if way == 0 else position + hop, n)

            @pl.when(jnp.logical_or(jnp.logical_not(last), mine))
            def _():
                ring_copy(way, hop, c).wait_recv()

            @pl.when(jnp.logical_and(hop < hops, jnp.logical_or(hop + 1 < hops, mine)))
            def _():
                ring_copy(way, hop + 1, c).start()

        @pl.loop(0, 2)
        def _(way):
            mine = low == (way == 0)

            @pl.when(jnp.logical_or(jnp.logical_not(last), mine))
            def _():
                compute(ring_member(jnp.where(way == 0, position - hop, position + hop), n), c)

    inverse = lax.rsqrt(
        jnp.sum(squares[...].reshape(chunks * chunk_rows, 128), axis=1, keepdims=True) * (1.0 / (n * width)) + NORM_EPS
    )
    cos, sin = cos_ref[...], sin_ref[...]
    projected = acc[...].reshape(chunks * chunk_rows, qw + kw + vw) * inverse
    for h in range(qw // HD):
        q = projected[:, h * HD : (h + 1) * HD]
        q_out[:, h * HD : (h + 1) * HD] = (q * cos + swap_pairs(q) * sin).astype(jnp.bfloat16)

    lane = lax.broadcasted_iota(jnp.int32, (HD, kw), 1)
    source = lax.broadcasted_iota(jnp.int32, (HD, kw), 0)
    pick = (source == (me * kw + lane) // (2 * KV_HEADS) * 2 + lane % 2).astype(jnp.float32)
    nn = (((1,), (0,)), ((), ()))
    k_cos = lax.dot_general(cos, pick, nn, precision=lax.Precision.HIGHEST, preferred_element_type=jnp.float32)
    k_sin = lax.dot_general(sin, pick, nn, precision=lax.Precision.HIGHEST, preferred_element_type=jnp.float32)
    k = projected[:, qw : qw + kw]
    k_rot = (k * k_cos + swap_pairs(k) * k_sin).astype(jnp.bfloat16)
    v_bf = projected[:, qw + kw :].astype(jnp.bfloat16)
    per_head = kw // KV_HEADS
    target = lax.broadcasted_iota(jnp.int32, (kw, kw), 0)
    origin_row = lax.broadcasted_iota(jnp.int32, (kw, kw), 1)
    head, within = target // per_head, target % per_head
    order = (origin_row == (within // 2 * KV_HEADS + head) * 2 + within % 2).astype(jnp.bfloat16)
    nt = (((1,), (1,)), ((), ()))
    k_out[...] = lax.dot_general(order, k_rot, nt, preferred_element_type=jnp.float32).astype(jnp.bfloat16)
    v_out[...] = lax.dot_general(order, v_bf, nt, preferred_element_type=jnp.float32).astype(jnp.bfloat16)
    for j in range(n):
        resid_out[:, j * width : (j + 1) * width] = x_all[j, me]

    for c in range(chunks):
        shift_copy(c).wait_send()

    @pl.loop(0, hops * chunks)
    def _(i):
        hop = i // chunks + 1
        c = lax.rem(i, chunks)
        for way in range(2):
            mine = (c < chunks // 2) if way == 0 else (c >= chunks // 2)

            @pl.when(jnp.logical_or(hop < hops, mine))
            def _():
                ring_copy(way, hop, c).wait_send()


def scatter_kernel(
    n, pieces, q_ref, k_ref, v_ref, w_hbm, resid_ref,
    attended_ref, stream_ref,
    w_out, context, running, w_sem, send_sem, recv_sem,
):
    me = lax.axis_index("mp")
    position = ring_position(me, n)
    right, left = ring_member(position + 1, n), ring_member(position - 1, n)
    rows = q_ref.shape[1]
    length = n * rows
    heads = q_ref.shape[2] // HD
    width = running.shape[4]
    w_copy = pltpu.make_async_copy(w_hbm, w_out, w_sem)
    w_copy.start()

    barrier = pltpu.get_barrier_semaphore()
    for partner in (right, left):
        pl.semaphore_signal(barrier, inc=1, device_id={"mp": partner}, device_id_type=MESH)

    scale = 1.0 / math.sqrt(HD)

    def attend(block):
        row = lax.broadcasted_iota(jnp.int32, (rows, length), 0) + block * rows
        column = lax.broadcasted_iota(jnp.int32, (rows, length), 1)
        for h in range(heads):
            q = q_ref[block, :, h * HD : (h + 1) * HD]
            scores = lax.dot_general(
                q, k_ref[...], (((1,), (0,)), ((), ())), preferred_element_type=jnp.float32
            ) * scale
            scores = jnp.where(row >= column, scores, -1e30)
            exponent = jnp.exp(scores - jnp.max(scores, axis=1, keepdims=True))
            probs = (exponent / jnp.sum(exponent, axis=1, keepdims=True)).astype(jnp.bfloat16)
            context[block, :, h * HD : (h + 1) * HD] = lax.dot_general(
                probs, v_ref[...], (((1,), (1,)), ((), ())), preferred_element_type=jnp.float32
            ).astype(jnp.bfloat16)

    def block_of(way, step):
        return ring_member(position - 1 - step if way == 0 else position + 1 + step, n)

    def term(way, step, piece):
        start = (way * pieces + piece) * width
        return jnp.dot(
            context[block_of(way, step)], w_out[:, start : start + width], preferred_element_type=jnp.float32
        )

    def copy(way, step, piece):
        return pltpu.make_async_remote_copy(
            src_ref=running.at[way, step, piece],
            dst_ref=running.at[way, step + 1, piece],
            send_sem=send_sem.at[way, step, piece], recv_sem=recv_sem.at[way, step, piece],
            device_id={"mp": right if way == 0 else left}, device_id_type=MESH,
        )

    attend(block_of(0, 0))
    attend(block_of(1, 0))
    w_copy.wait()
    pl.semaphore_wait(barrier, 2)
    for piece in range(pieces):
        for way in range(2):
            running[way, 0, piece] = term(way, 0, piece).astype(jnp.bfloat16)
            copy(way, 0, piece).start()

    def ahead(step):
        @pl.when(step < n // 2)
        def _():
            attend(block_of(0, step))
            attend(block_of(1, step))

        @pl.when(step == n // 2)
        def _():
            attend(me)

    ahead(1)

    @pl.loop(1, n - 1)
    def _(step):
        for piece in range(pieces):
            for way in range(2):
                value = term(way, step, piece)
                copy(way, step - 1, piece).wait_recv()
                running[way, step, piece] = (running[way, step, piece].astype(jnp.float32) + value).astype(jnp.bfloat16)
                copy(way, step, piece).start()
        ahead(step + 1)

    for piece in range(pieces):
        for way in range(2):
            value = term(way, n - 1, piece)
            copy(way, n - 2, piece).wait_recv()
            value = running[way, n - 1, piece].astype(jnp.float32) + value
            columns = slice((way * pieces + piece) * width, (way * pieces + piece + 1) * width)
            attended_ref[:, columns] = value.astype(jnp.bfloat16)
            stream_ref[:, columns] = (resid_ref[:, columns].astype(jnp.float32) + value).astype(jnp.bfloat16)

    @pl.loop(0, n - 1)
    def _(step):
        for piece in range(pieces):
            for way in range(2):
                copy(way, step, piece).wait_send()


def rotary_tables(length):
    pair = (np.arange(HD) // 2).astype(np.float32)
    frequency = np.exp(pair * np.float32(-2.0 * math.log(ROPE_BASE) / HD)).astype(np.float32)
    angles = frequency[None, :] * np.arange(length, dtype=np.float32)[:, None]
    sign = np.where(np.arange(HD) % 2 == 0, -1.0, 1.0).astype(np.float32)
    return np.cos(angles).astype(np.float32), (np.sin(angles) * sign).astype(np.float32)


def local(arriving, norm_gain, w_query, w_key, w_value, w_out):
    n = lax.axis_size("mp")
    length, width = arriving.shape[1:]
    rows = length // n
    full = n * width
    chunks = 4 if n <= 8 else 2
    pieces = 4 if n <= 8 else 2
    qw, kw, vw = w_query.shape[1], w_key.shape[1], w_value.shape[1]
    cos, sin = rotary_tables(length)
    vmem = pl.BlockSpec(memory_space=pltpu.VMEM)
    anywhere = pl.BlockSpec(memory_space=pl.ANY)
    bf16, f32 = jnp.bfloat16, jnp.float32
    dma = pltpu.SemaphoreType.DMA
    q, k, v, resid = pl.pallas_call(
        functools.partial(gather_kernel, n, chunks),
        name="gather_project",
        out_shape=(
            jax.ShapeDtypeStruct((length, qw), bf16),
            jax.ShapeDtypeStruct((kw, length), bf16),
            jax.ShapeDtypeStruct((vw, length), bf16),
            jax.ShapeDtypeStruct((rows, full), bf16),
        ),
        in_specs=[anywhere, vmem, anywhere, anywhere, anywhere, vmem, vmem],
        out_specs=(vmem,) * 4,
        scratch_shapes=[
            pltpu.VMEM((n, n, rows, width), bf16),
            pltpu.VMEM((n, qw + kw + vw, width), bf16),
            pltpu.VMEM((chunks, length // chunks, qw + kw + vw), f32),
            pltpu.VMEM((chunks, length // chunks, 128), f32),
            dma((n, 3)),
            dma((chunks,)),
            dma((chunks,)),
            dma((2, n // 2, chunks)),
            dma((2, n // 2, chunks)),
        ],
        compiler_params=pltpu.CompilerParams(collective_id=0, has_side_effects=True, vmem_limit_bytes=VMEM_LIMIT),
    )(
        arriving[0].reshape(n, rows, width),
        norm_gain[0].astype(f32).reshape(n, 1, width),
        w_query[0], w_key[0], w_value[0], jnp.asarray(cos), jnp.asarray(sin),
    )
    per_head = kw // KV_HEADS
    sent = jnp.stack([k.reshape(KV_HEADS, per_head, length), v.reshape(KV_HEADS, per_head, length)], axis=1)
    local_heads = qw // HD
    group_size = local_heads * n // KV_HEADS
    if n != KV_HEADS:
        sent = sent[np.arange(n) * local_heads // group_size]
    got = lax.all_to_all(sent, "mp", 0, 0, tiled=True)
    key_head = got[:, 0].reshape(HD, length)
    value_head = got[:, 1].reshape(HD, length)
    attended, stream = pl.pallas_call(
        functools.partial(scatter_kernel, n, pieces),
        name="attend_scatter",
        out_shape=(jax.ShapeDtypeStruct((rows, full), bf16),) * 2,
        in_specs=[vmem, vmem, vmem, anywhere, vmem],
        out_specs=(vmem, vmem),
        scratch_shapes=[
            pltpu.VMEM((qw, full), bf16),
            pltpu.VMEM((n, rows, qw), bf16),
            pltpu.VMEM((2, n, pieces, rows, full // (2 * pieces)), bf16),
            dma(()),
            dma((2, n - 1, pieces)),
            dma((2, n - 1, pieces)),
        ],
        compiler_params=pltpu.CompilerParams(collective_id=1, has_side_effects=True, vmem_limit_bytes=VMEM_LIMIT),
    )(q.reshape(n, rows, qw), key_head, value_head, w_out[0], resid)
    return (attended[None], stream[None])


def solution(mesh):
    return jax.shard_map(
        local,
        mesh=mesh,
        in_specs=(
            P("section", None, "mp"),
            P("section", None),
            P("section", "mp", None),
            P("section", "mp", None),
            P("section", "mp", None),
            P("section", "mp", None),
        ),
        out_specs=(P("section", "mp", None), P("section", "mp", None)),
        check_vma=False,
    )
```

```python
import functools
import math

import jax
import jax.numpy as jnp
import numpy as np
from jax import lax
from jax.experimental import pallas as pl
from jax.experimental.pallas import tpu as pltpu
from jax.sharding import PartitionSpec as P

HD = 128
KV_HEADS = 8
ROPE_BASE = 500000.0
NORM_EPS = 1e-05
MESH = pl.DeviceIdType.MESH
VMEM_LIMIT = 64000000


def ring_position(member, n):
    return jnp.where(member % 2 == 0, member // 2, n - 1 - member // 2)


def ring_member(position, n):
    position = lax.rem(position + 2 * n, n)
    return jnp.where(position < n // 2, 2 * position, 2 * (n - 1 - position) + 1)


def swap_pairs(x):
    lane = lax.broadcasted_iota(jnp.int32, x.shape, 1)
    width = x.shape[1]
    return jnp.where(lane % 2 == 0, pltpu.roll(x, width - 1, 1), pltpu.roll(x, 1, 1))


def layer_kernel(
    n, chunks, pieces, arriving, gain, wq, wk, wv, w_hbm, cos_ref, sin_ref,
    attended_ref, stream_ref,
    x_all, weights, acc, squares, sent, got, heads_kv, key_head, value_head, q_ref, w_out, context, running,
    w_sem, wo_sem, shift_send, shift_recv, ring_send, ring_recv, kv_send, kv_recv, send_sem, recv_sem,
):
    sections = lax.axis_size("section")
    section = lax.axis_index("section")
    me = lax.axis_index("mp")
    position = ring_position(me, n)
    right, left = ring_member(position + 1, n), ring_member(position - 1, n)
    following, previous = lax.rem(section + 1, sections), lax.rem(section + sections - 1, sections)
    hops = n // 2
    per = n // chunks
    rows, width = x_all.shape[2:]
    length = n * rows
    chunk_rows = per * rows
    qw, kw, vw = wq.shape[0], wk.shape[0], wv.shape[0]
    heads = qw // HD
    group_size = heads * n // KV_HEADS
    nn = (((1,), (0,)), ((), ()))
    nt = (((1,), (1,)), ((), ()))

    barrier = pltpu.get_barrier_semaphore()
    for step in range(1, n):
        pl.semaphore_signal(barrier, inc=1, device_id={"mp": lax.rem(me + step, n)}, device_id_type=MESH)
    for partner in (following, previous):
        pl.semaphore_signal(barrier, inc=1, device_id={"section": partner}, device_id_type=MESH)

    def weight_copy(j, part):
        src, start, size = ((wq, 0, qw), (wk, qw, kw), (wv, qw + kw, vw))[part]
        return pltpu.make_async_copy(
            src.at[:, pl.ds(j * width, width)], weights.at[j, pl.ds(start, size)], w_sem.at[j, part]
        )

    def shift_copy(c):
        return pltpu.make_async_remote_copy(
            src_ref=arriving.at[pl.ds(c * per, per)],
            dst_ref=x_all.at[me, pl.ds(c * per, per)],
            send_sem=shift_send.at[c], recv_sem=shift_recv.at[c],
            device_id={"section": following}, device_id_type=MESH,
        )

    def ring_copy(way, hop, c):
        origin = ring_member(position - (hop - 1) if way == 0 else position + (hop - 1), n)
        return pltpu.make_async_remote_copy(
            src_ref=x_all.at[origin, pl.ds(c * per, per)],
            dst_ref=x_all.at[origin, pl.ds(c * per, per)],
            send_sem=ring_send.at[way, hop - 1, c], recv_sem=ring_recv.at[way, hop - 1, c],
            device_id={"mp": right if way == 0 else left}, device_id_type=MESH,
        )

    pl.semaphore_wait(barrier, n + 1)
    for c in range(chunks):
        shift_copy(c).start()
    for j in range(n):
        for part in range(3):
            weight_copy(j, part).start()
    acc[...] = jnp.zeros_like(acc)
    squares[...] = jnp.zeros_like(squares)

    def compute(slot, c):
        x = x_all[slot, pl.ds(c * per, per)].astype(jnp.float32).reshape(chunk_rows, width)
        total = x[:, :128] * x[:, :128]
        for g in range(1, width // 128):
            part = x[:, g * 128 : (g + 1) * 128]
            total = total + part * part
        squares[c] += total
        scaled = (x * gain[slot].astype(jnp.float32)).astype(jnp.bfloat16)
        acc[c] += lax.dot_general(scaled, weights[slot], nt, preferred_element_type=jnp.float32)

    for c in range(chunks):
        shift_copy(c).wait_recv()
        ring_copy(0, 1, c).start()
        ring_copy(1, 1, c).start()
    for j in range(n):
        for part in range(3):
            weight_copy(j, part).wait()
    wo_copy = pltpu.make_async_copy(w_hbm, w_out, wo_sem)
    wo_copy.start()

    @pl.loop(0, chunks)
    def _(c):
        compute(me, c)

    cos, sin = cos_ref[...], sin_ref[...]
    lane = lax.broadcasted_iota(jnp.int32, (HD, kw), 1)
    source = lax.broadcasted_iota(jnp.int32, (HD, kw), 0)
    pick = (source == (me * kw + lane) // (2 * KV_HEADS) * 2 + lane % 2).astype(jnp.float32)
    k_cos = lax.dot_general(cos, pick, nn, precision=lax.Precision.HIGHEST, preferred_element_type=jnp.float32)
    k_sin = lax.dot_general(sin, pick, nn, precision=lax.Precision.HIGHEST, preferred_element_type=jnp.float32)
    per_head = kw // KV_HEADS
    target = lax.broadcasted_iota(jnp.int32, (kw, kw), 0)
    origin_row = lax.broadcasted_iota(jnp.int32, (kw, kw), 1)
    head, within = target // per_head, target % per_head
    order = (origin_row == (within // 2 * KV_HEADS + head) * 2 + within % 2).astype(jnp.bfloat16)

    @pl.loop(0, hops * chunks)
    def _(i):
        hop = i // chunks + 1
        c = lax.rem(i, chunks)
        last = hop == hops
        low = c < chunks // 2
        for way in range(2):
            mine = low if way == 0 else jnp.logical_not(low)

            @pl.when(jnp.logical_or(jnp.logical_not(last), mine))
            def _():
                ring_copy(way, hop, c).wait_recv()

            @pl.when(jnp.logical_and(hop < hops, jnp.logical_or(hop + 1 < hops, mine)))
            def _():
                ring_copy(way, hop + 1, c).start()

        @pl.loop(0, 2)
        def _(way):
            mine = low == (way == 0)

            @pl.when(jnp.logical_or(jnp.logical_not(last), mine))
            def _():
                compute(ring_member(jnp.where(way == 0, position - hop, position + hop), n), c)

    inverse = lax.rsqrt(
        jnp.sum(squares[...].reshape(length, 128), axis=1, keepdims=True) * (1.0 / (n * width)) + NORM_EPS
    )
    k = acc[:, :, qw : qw + kw].reshape(length, kw) * inverse
    k_rot = (k * k_cos + swap_pairs(k) * k_sin).astype(jnp.bfloat16)
    v_bf = (acc[:, :, qw + kw :].reshape(length, vw) * inverse).astype(jnp.bfloat16)
    for part, rotated in enumerate((k_rot, v_bf)):
        ordered = lax.dot_general(order, rotated, nt, preferred_element_type=jnp.float32)
        for h in range(KV_HEADS):
            sent[h, part] = ordered[h * per_head : (h + 1) * per_head].astype(jnp.bfloat16)

    def kv_copy(step):
        other = lax.rem(me + step, n)
        return pltpu.make_async_remote_copy(
            src_ref=sent.at[other * heads // group_size], dst_ref=got.at[me],
            send_sem=kv_send.at[step - 1], recv_sem=kv_recv.at[step - 1],
            device_id={"mp": other}, device_id_type=MESH,
        )

    for step in range(1, n):
        kv_copy(step).start()
    got[me] = sent[me * heads // group_size]
    for h in range(heads):
        q = acc[:, :, h * HD : (h + 1) * HD].reshape(length, HD) * inverse
        q_ref[:, :, h * HD : (h + 1) * HD] = (
            (q * cos + swap_pairs(q) * sin).reshape(n, rows, HD).astype(jnp.bfloat16)
        )
    for step in range(1, n):
        kv_copy(step).wait_recv()
    for j in range(n):
        for part in range(2):
            heads_kv[part, j * per_head : (j + 1) * per_head] = got[j, part].astype(jnp.float32)
    key_head[...] = heads_kv[0].astype(jnp.bfloat16)
    value_head[...] = heads_kv[1].astype(jnp.bfloat16)

    piece_width = running.shape[4]
    scale = 1.0 / math.sqrt(HD)

    def attend(block):
        row = lax.broadcasted_iota(jnp.int32, (rows, length), 0) + block * rows
        column = lax.broadcasted_iota(jnp.int32, (rows, length), 1)
        for h in range(heads):
            q = q_ref[block, :, h * HD : (h + 1) * HD]
            scores = lax.dot_general(q, key_head[...], nn, preferred_element_type=jnp.float32) * scale
            scores = jnp.where(row >= column, scores, -1e30)
            exponent = jnp.exp(scores - jnp.max(scores, axis=1, keepdims=True))
            probs = (exponent / jnp.sum(exponent, axis=1, keepdims=True)).astype(jnp.bfloat16)
            context[block, :, h * HD : (h + 1) * HD] = lax.dot_general(
                probs, value_head[...], nt, preferred_element_type=jnp.float32
            ).astype(jnp.bfloat16)

    def block_of(way, step):
        return ring_member(position - 1 - step if way == 0 else position + 1 + step, n)

    def term(way, step, piece):
        start = (way * pieces + piece) * piece_width
        return jnp.dot(
            context[block_of(way, step)], w_out[:, start : start + piece_width], preferred_element_type=jnp.float32
        )

    def sum_copy(way, step, piece):
        return pltpu.make_async_remote_copy(
            src_ref=running.at[way, step, piece],
            dst_ref=running.at[way, step + 1, piece],
            send_sem=send_sem.at[way, step, piece], recv_sem=recv_sem.at[way, step, piece],
            device_id={"mp": right if way == 0 else left}, device_id_type=MESH,
        )

    wo_copy.wait()
    for way in range(2):
        attend(block_of(way, 0))
        for piece in range(pieces):
            running[way, 0, piece] = term(way, 0, piece).astype(jnp.bfloat16)
            sum_copy(way, 0, piece).start()

    def ahead(step):
        @pl.when(step < n // 2)
        def _():
            attend(block_of(0, step))
            attend(block_of(1, step))

        @pl.when(step == n // 2)
        def _():
            attend(me)

    ahead(1)

    @pl.loop(1, n - 1)
    def _(step):
        for piece in range(pieces):
            for way in range(2):
                value = term(way, step, piece)
                sum_copy(way, step - 1, piece).wait_recv()
                running[way, step, piece] = (running[way, step, piece].astype(jnp.float32) + value).astype(jnp.bfloat16)
                sum_copy(way, step, piece).start()
        ahead(step + 1)

    for j in range(n):
        stream_ref[:, j * width : (j + 1) * width] = x_all[j, me]
    for piece in range(pieces):
        for way in range(2):
            value = term(way, n - 1, piece)
            sum_copy(way, n - 2, piece).wait_recv()
            value = running[way, n - 1, piece].astype(jnp.float32) + value
            columns = slice((way * pieces + piece) * piece_width, (way * pieces + piece + 1) * piece_width)
            attended_ref[:, columns] = value.astype(jnp.bfloat16)
            stream_ref[:, columns] = (stream_ref[:, columns].astype(jnp.float32) + value).astype(jnp.bfloat16)

    for c in range(chunks):
        shift_copy(c).wait_send()
    for step in range(1, n):
        kv_copy(step).wait_send()

    @pl.loop(0, hops * chunks)
    def _(i):
        hop = i // chunks + 1
        c = lax.rem(i, chunks)
        for way in range(2):
            mine = (c < chunks // 2) if way == 0 else (c >= chunks // 2)

            @pl.when(jnp.logical_or(hop < hops, mine))
            def _():
                ring_copy(way, hop, c).wait_send()

    @pl.loop(0, n - 1)
    def _(step):
        for piece in range(pieces):
            for way in range(2):
                sum_copy(way, step, piece).wait_send()


def rotary_tables(length):
    pair = (np.arange(HD) // 2).astype(np.float32)
    frequency = np.exp(pair * np.float32(-2.0 * math.log(ROPE_BASE) / HD)).astype(np.float32)
    angles = frequency[None, :] * np.arange(length, dtype=np.float32)[:, None]
    sign = np.where(np.arange(HD) % 2 == 0, -1.0, 1.0).astype(np.float32)
    return np.cos(angles).astype(np.float32), (np.sin(angles) * sign).astype(np.float32)


def local(arriving, norm_gain, w_query, w_key, w_value, w_out):
    n = lax.axis_size("mp")
    length, width = arriving.shape[1:]
    rows = length // n
    full = n * width
    chunks = 8 if n <= 8 else 2
    pieces = 4 if n <= 8 else 2
    qw, kw, vw = w_query.shape[1], w_key.shape[1], w_value.shape[1]
    cos, sin = rotary_tables(length)
    vmem = pl.BlockSpec(memory_space=pltpu.VMEM)
    anywhere = pl.BlockSpec(memory_space=pl.ANY)
    bf16, f32 = jnp.bfloat16, jnp.float32
    dma = pltpu.SemaphoreType.DMA
    attended, stream = pl.pallas_call(
        functools.partial(layer_kernel, n, chunks, pieces),
        name="layer",
        out_shape=(jax.ShapeDtypeStruct((rows, full), bf16),) * 2,
        in_specs=[anywhere, vmem, anywhere, anywhere, anywhere, anywhere, vmem, vmem],
        out_specs=(vmem, vmem),
        scratch_shapes=[
            pltpu.VMEM((n, n, rows, width), bf16),
            pltpu.VMEM((n, qw + kw + vw, width), bf16),
            pltpu.VMEM((chunks, length // chunks, qw + kw + vw), f32),
            pltpu.VMEM((chunks, length // chunks, 128), f32),
            pltpu.VMEM((KV_HEADS, 2, kw // KV_HEADS, length), bf16),
            pltpu.VMEM((n, 2, kw // KV_HEADS, length), bf16),
            pltpu.VMEM((2, HD, length), f32),
            pltpu.VMEM((HD, length), bf16),
            pltpu.VMEM((HD, length), bf16),
            pltpu.VMEM((n, rows, qw), bf16),
            pltpu.VMEM((qw, full), bf16),
            pltpu.VMEM((n, rows, qw), bf16),
            pltpu.VMEM((2, n, pieces, rows, full // (2 * pieces)), bf16),
            dma((n, 3)),
            dma(()),
            dma((chunks,)),
            dma((chunks,)),
            dma((2, n // 2, chunks)),
            dma((2, n // 2, chunks)),
            dma((n - 1,)),
            dma((n - 1,)),
            dma((2, n - 1, pieces)),
            dma((2, n - 1, pieces)),
        ],
        compiler_params=pltpu.CompilerParams(collective_id=0, has_side_effects=True, vmem_limit_bytes=VMEM_LIMIT),
    )(
        arriving[0].reshape(n, rows, width),
        norm_gain[0].reshape(n, 1, width),
        w_query[0], w_key[0], w_value[0], w_out[0], jnp.asarray(cos), jnp.asarray(sin),
    )
    return (attended[None], stream[None])


def solution(mesh):
    return jax.shard_map(
        local,
        mesh=mesh,
        in_specs=(
            P("section", None, "mp"),
            P("section", None),
            P("section", "mp", None),
            P("section", "mp", None),
            P("section", "mp", None),
            P("section", "mp", None),
        ),
        out_specs=(P("section", "mp", None), P("section", "mp", None)),
        check_vma=False,
    )
```

```python
import functools
import math

import jax
import jax.numpy as jnp
import numpy as np
from jax import lax
from jax.experimental import pallas as pl
from jax.experimental.pallas import tpu as pltpu
from jax.sharding import PartitionSpec as P

HD = 128
KV_HEADS = 8
ROPE_BASE = 500000.0
NORM_EPS = 1e-05
MESH = pl.DeviceIdType.MESH
VMEM_LIMIT = 52000000


def ring_position(member, n):
    return jnp.where(member % 2 == 0, member // 2, n - 1 - member // 2)


def ring_member(position, n):
    position = lax.rem(position + 2 * n, n)
    return jnp.where(position < n // 2, 2 * position, 2 * (n - 1 - position) + 1)


def swap_pairs(x):
    lane = lax.broadcasted_iota(jnp.int32, x.shape, 1)
    width = x.shape[1]
    return jnp.where(lane % 2 == 0, pltpu.roll(x, width - 1, 1), pltpu.roll(x, 1, 1))


def layer_kernel(
    n, chunks, pieces, arriving, gain_hbm, wq, wk, wv, w_hbm, tables_hbm,
    attended_ref, stream_ref,
    staged, gain, tables, x_all, weights, acc, squares, sent, got, heads_kv, key_head, value_head, q_ref, w_out, context, running,
    stage_sem, gain_sem, tables_sem, w_sem, wo_sem, shift_send, shift_recv, ring_send, ring_recv, kv_send, kv_recv, send_sem, recv_sem,
):
    sections = lax.axis_size("section")
    section = lax.axis_index("section")
    me = lax.axis_index("mp")
    position = ring_position(me, n)
    right, left = ring_member(position + 1, n), ring_member(position - 1, n)
    following, previous = lax.rem(section + 1, sections), lax.rem(section + sections - 1, sections)
    hops = n // 2
    per = n // chunks
    rows, width = x_all.shape[2:]
    length = n * rows
    chunk_rows = per * rows
    qw, kw, vw = wq.shape[0], wk.shape[0], wv.shape[0]
    heads = qw // HD
    group_size = heads * n // KV_HEADS
    nn = (((1,), (0,)), ((), ()))
    nt = (((1,), (1,)), ((), ()))

    stage = pltpu.make_async_copy(arriving, staged, stage_sem)
    stage.start()
    gain_copy = pltpu.make_async_copy(gain_hbm, gain, gain_sem)
    gain_copy.start()
    tables_copy = pltpu.make_async_copy(tables_hbm, tables, tables_sem)
    tables_copy.start()
    barrier = pltpu.get_barrier_semaphore()
    for step in range(1, n):
        pl.semaphore_signal(barrier, inc=1, device_id={"mp": lax.rem(me + step, n)}, device_id_type=MESH)
    for partner in (following, previous):
        pl.semaphore_signal(barrier, inc=1, device_id={"section": partner}, device_id_type=MESH)

    def weight_copy(j, part):
        src, start, size = ((wq, 0, qw), (wk, qw, kw), (wv, qw + kw, vw))[part]
        return pltpu.make_async_copy(
            src.at[:, pl.ds(j * width, width)], weights.at[j, pl.ds(start, size)], w_sem.at[j, part]
        )

    def shift_copy(c):
        return pltpu.make_async_remote_copy(
            src_ref=staged.at[pl.ds(c * per, per)],
            dst_ref=x_all.at[me, pl.ds(c * per, per)],
            send_sem=shift_send.at[c], recv_sem=shift_recv.at[c],
            device_id={"section": following}, device_id_type=MESH,
        )

    def ring_copy(way, hop, c):
        origin = ring_member(position - (hop - 1) if way == 0 else position + (hop - 1), n)
        return pltpu.make_async_remote_copy(
            src_ref=x_all.at[origin, pl.ds(c * per, per)],
            dst_ref=x_all.at[origin, pl.ds(c * per, per)],
            send_sem=ring_send.at[way, hop - 1, c], recv_sem=ring_recv.at[way, hop - 1, c],
            device_id={"mp": right if way == 0 else left}, device_id_type=MESH,
        )

    for j in range(n):
        for part in range(3):
            weight_copy(j, part).start()
    stage.wait()
    pl.semaphore_wait(barrier, n + 1)
    for c in range(chunks):
        shift_copy(c).start()
    acc[...] = jnp.zeros_like(acc)
    squares[...] = jnp.zeros_like(squares)

    def compute(slot, c):
        x = x_all[slot, pl.ds(c * per, per)].astype(jnp.float32).reshape(chunk_rows, width)
        total = x[:, :128] * x[:, :128]
        for g in range(1, width // 128):
            part = x[:, g * 128 : (g + 1) * 128]
            total = total + part * part
        squares[c] += total
        scaled = (x * gain[slot].astype(jnp.float32)).astype(jnp.bfloat16)
        acc[c] += lax.dot_general(scaled, weights[slot], nt, preferred_element_type=jnp.float32)

    for c in range(chunks):
        shift_copy(c).wait_recv()
        ring_copy(0, 1, c).start()
        ring_copy(1, 1, c).start()
    for j in range(n):
        for part in range(3):
            weight_copy(j, part).wait()
    gain_copy.wait()
    tables_copy.wait()
    wo_copy = pltpu.make_async_copy(w_hbm, w_out, wo_sem)
    wo_copy.start()

    @pl.loop(0, chunks)
    def _(c):
        compute(me, c)

    cos, sin = tables[0], tables[1]
    lane = lax.broadcasted_iota(jnp.int32, (HD, kw), 1)
    source = lax.broadcasted_iota(jnp.int32, (HD, kw), 0)
    pick = (source == (me * kw + lane) // (2 * KV_HEADS) * 2 + lane % 2).astype(jnp.float32)
    k_cos = lax.dot_general(cos, pick, nn, precision=lax.Precision.HIGHEST, preferred_element_type=jnp.float32)
    k_sin = lax.dot_general(sin, pick, nn, precision=lax.Precision.HIGHEST, preferred_element_type=jnp.float32)
    per_head = kw // KV_HEADS
    target = lax.broadcasted_iota(jnp.int32, (kw, kw), 0)
    origin_row = lax.broadcasted_iota(jnp.int32, (kw, kw), 1)
    head, within = target // per_head, target % per_head
    order = (origin_row == (within // 2 * KV_HEADS + head) * 2 + within % 2).astype(jnp.bfloat16)

    @pl.loop(0, hops * chunks)
    def _(i):
        hop = i // chunks + 1
        c = lax.rem(i, chunks)
        last = hop == hops
        low = c < chunks // 2
        for way in range(2):
            mine = low if way == 0 else jnp.logical_not(low)

            @pl.when(jnp.logical_or(jnp.logical_not(last), mine))
            def _():
                ring_copy(way, hop, c).wait_recv()

            @pl.when(jnp.logical_and(hop < hops, jnp.logical_or(hop + 1 < hops, mine)))
            def _():
                ring_copy(way, hop + 1, c).start()

        @pl.loop(0, 2)
        def _(way):
            mine = low == (way == 0)

            @pl.when(jnp.logical_or(jnp.logical_not(last), mine))
            def _():
                compute(ring_member(jnp.where(way == 0, position - hop, position + hop), n), c)

    inverse = lax.rsqrt(
        jnp.sum(squares[...].reshape(length, 128), axis=1, keepdims=True) * (1.0 / (n * width)) + NORM_EPS
    )
    k = acc[:, :, qw : qw + kw].reshape(length, kw) * inverse
    k_rot = (k * k_cos + swap_pairs(k) * k_sin).astype(jnp.bfloat16)
    v_bf = (acc[:, :, qw + kw :].reshape(length, vw) * inverse).astype(jnp.bfloat16)
    for part, rotated in enumerate((k_rot, v_bf)):
        ordered = lax.dot_general(order, rotated, nt, preferred_element_type=jnp.float32)
        for h in range(KV_HEADS):
            sent[h, part] = ordered[h * per_head : (h + 1) * per_head].astype(jnp.bfloat16)

    def kv_copy(step):
        other = lax.rem(me + step, n)
        return pltpu.make_async_remote_copy(
            src_ref=sent.at[other * heads // group_size], dst_ref=got.at[me],
            send_sem=kv_send.at[step - 1], recv_sem=kv_recv.at[step - 1],
            device_id={"mp": other}, device_id_type=MESH,
        )

    for step in range(1, n):
        kv_copy(step).start()
    got[me] = sent[me * heads // group_size]
    for h in range(heads):
        q = acc[:, :, h * HD : (h + 1) * HD].reshape(length, HD) * inverse
        q_ref[:, :, h * HD : (h + 1) * HD] = (
            (q * cos + swap_pairs(q) * sin).reshape(n, rows, HD).astype(jnp.bfloat16)
        )
    for step in range(1, n):
        kv_copy(step).wait_recv()
    for j in range(n):
        for part in range(2):
            heads_kv[part, j * per_head : (j + 1) * per_head] = got[j, part].astype(jnp.float32)
    key_head[...] = heads_kv[0].astype(jnp.bfloat16)
    value_head[...] = heads_kv[1].astype(jnp.bfloat16)

    piece_width = running.shape[4]
    scale = 1.0 / math.sqrt(HD)

    def attend(block):
        row = lax.broadcasted_iota(jnp.int32, (rows, length), 0) + block * rows
        column = lax.broadcasted_iota(jnp.int32, (rows, length), 1)
        for h in range(heads):
            q = q_ref[block, :, h * HD : (h + 1) * HD]
            scores = lax.dot_general(q, key_head[...], nn, preferred_element_type=jnp.float32) * scale
            scores = jnp.where(row >= column, scores, -1e30)
            exponent = jnp.exp(scores - jnp.max(scores, axis=1, keepdims=True))
            probs = (exponent / jnp.sum(exponent, axis=1, keepdims=True)).astype(jnp.bfloat16)
            context[block, :, h * HD : (h + 1) * HD] = lax.dot_general(
                probs, value_head[...], nt, preferred_element_type=jnp.float32
            ).astype(jnp.bfloat16)

    def block_of(way, step):
        return ring_member(position - 1 - step if way == 0 else position + 1 + step, n)

    def term(way, step, piece):
        start = (way * pieces + piece) * piece_width
        return jnp.dot(
            context[block_of(way, step)], w_out[:, start : start + piece_width], preferred_element_type=jnp.float32
        )

    def sum_copy(way, step, piece):
        return pltpu.make_async_remote_copy(
            src_ref=running.at[way, step, piece],
            dst_ref=running.at[way, step + 1, piece],
            send_sem=send_sem.at[way, step, piece], recv_sem=recv_sem.at[way, step, piece],
            device_id={"mp": right if way == 0 else left}, device_id_type=MESH,
        )

    wo_copy.wait()
    for way in range(2):
        attend(block_of(way, 0))
        for piece in range(pieces):
            running[way, 0, piece] = term(way, 0, piece).astype(jnp.bfloat16)
            sum_copy(way, 0, piece).start()

    def ahead(step):
        @pl.when(step < n // 2)
        def _():
            attend(block_of(0, step))
            attend(block_of(1, step))

        @pl.when(step == n // 2)
        def _():
            attend(me)

    ahead(1)

    @pl.loop(1, n - 1)
    def _(step):
        for piece in range(pieces):
            for way in range(2):
                value = term(way, step, piece)
                sum_copy(way, step - 1, piece).wait_recv()
                running[way, step, piece] = (running[way, step, piece].astype(jnp.float32) + value).astype(jnp.bfloat16)
                sum_copy(way, step, piece).start()
        ahead(step + 1)

    for j in range(n):
        stream_ref[:, j * width : (j + 1) * width] = x_all[j, me]
    for piece in range(pieces):
        for way in range(2):
            value = term(way, n - 1, piece)
            sum_copy(way, n - 2, piece).wait_recv()
            value = running[way, n - 1, piece].astype(jnp.float32) + value
            columns = slice((way * pieces + piece) * piece_width, (way * pieces + piece + 1) * piece_width)
            attended_ref[:, columns] = value.astype(jnp.bfloat16)
            stream_ref[:, columns] = (stream_ref[:, columns].astype(jnp.float32) + value).astype(jnp.bfloat16)

    for c in range(chunks):
        shift_copy(c).wait_send()
    for step in range(1, n):
        kv_copy(step).wait_send()

    @pl.loop(0, hops * chunks)
    def _(i):
        hop = i // chunks + 1
        c = lax.rem(i, chunks)
        for way in range(2):
            mine = (c < chunks // 2) if way == 0 else (c >= chunks // 2)

            @pl.when(jnp.logical_or(hop < hops, mine))
            def _():
                ring_copy(way, hop, c).wait_send()

    @pl.loop(0, n - 1)
    def _(step):
        for piece in range(pieces):
            for way in range(2):
                sum_copy(way, step, piece).wait_send()


def rotary_tables(length):
    pair = (np.arange(HD) // 2).astype(np.float32)
    frequency = np.exp(pair * np.float32(-2.0 * math.log(ROPE_BASE) / HD)).astype(np.float32)
    angles = frequency[None, :] * np.arange(length, dtype=np.float32)[:, None]
    sign = np.where(np.arange(HD) % 2 == 0, -1.0, 1.0).astype(np.float32)
    return np.stack([np.cos(angles), np.sin(angles) * sign]).astype(np.float32)


def local(arriving, norm_gain, w_query, w_key, w_value, w_out):
    n = lax.axis_size("mp")
    length, width = arriving.shape[1:]
    rows = length // n
    full = n * width
    chunks = 8 if n <= 8 else 2
    pieces = 4 if n <= 8 else 2
    qw, kw, vw = w_query.shape[1], w_key.shape[1], w_value.shape[1]
    tables = rotary_tables(length)
    vmem = pl.BlockSpec(memory_space=pltpu.VMEM)
    hbm = pl.BlockSpec(memory_space=pltpu.HBM)
    bf16, f32 = jnp.bfloat16, jnp.float32
    dma = pltpu.SemaphoreType.DMA
    attended, stream = pl.pallas_call(
        functools.partial(layer_kernel, n, chunks, pieces),
        name="layer",
        out_shape=(pltpu.VMEM((rows, full), bf16),) * 2,
        in_specs=[hbm] * 7,
        out_specs=(vmem, vmem),
        scratch_shapes=[
            pltpu.VMEM((n, rows, width), bf16),
            pltpu.VMEM((n, 1, width), bf16),
            pltpu.VMEM((2, length, HD), f32),
            pltpu.VMEM((n, n, rows, width), bf16),
            pltpu.VMEM((n, qw + kw + vw, width), bf16),
            pltpu.VMEM((chunks, length // chunks, qw + kw + vw), f32),
            pltpu.VMEM((chunks, length // chunks, 128), f32),
            pltpu.VMEM((KV_HEADS, 2, kw // KV_HEADS, length), bf16),
            pltpu.VMEM((n, 2, kw // KV_HEADS, length), bf16),
            pltpu.VMEM((2, HD, length), f32),
            pltpu.VMEM((HD, length), bf16),
            pltpu.VMEM((HD, length), bf16),
            pltpu.VMEM((n, rows, qw), bf16),
            pltpu.VMEM((qw, full), bf16),
            pltpu.VMEM((n, rows, qw), bf16),
            pltpu.VMEM((2, n, pieces, rows, full // (2 * pieces)), bf16),
            dma(()),
            dma(()),
            dma(()),
            dma((n, 3)),
            dma(()),
            dma((chunks,)),
            dma((chunks,)),
            dma((2, n // 2, chunks)),
            dma((2, n // 2, chunks)),
            dma((n - 1,)),
            dma((n - 1,)),
            dma((2, n - 1, pieces)),
            dma((2, n - 1, pieces)),
        ],
        compiler_params=pltpu.CompilerParams(collective_id=0, has_side_effects=True, vmem_limit_bytes=VMEM_LIMIT),
    )(
        arriving[0].reshape(n, rows, width),
        norm_gain[0].reshape(n, 1, width),
        w_query[0], w_key[0], w_value[0], w_out[0], jnp.asarray(tables),
    )
    return (attended[None], stream[None])


def solution(mesh):
    return jax.shard_map(
        local,
        mesh=mesh,
        in_specs=(
            P("section", None, "mp"),
            P("section", None),
            P("section", "mp", None),
            P("section", "mp", None),
            P("section", "mp", None),
            P("section", "mp", None),
        ),
        out_specs=(P("section", "mp", None), P("section", "mp", None)),
        check_vma=False,
    )
```

```python
import functools
import math

import jax
import jax.numpy as jnp
import numpy as np
from jax import lax
from jax.experimental import pallas as pl
from jax.experimental.pallas import tpu as pltpu
from jax.sharding import PartitionSpec as P

HD = 128
KV_HEADS = 8
ROPE_BASE = 500000.0
NORM_EPS = 1e-05
MESH = pl.DeviceIdType.MESH
VMEM_LIMIT = 63500000


def ring_position(member, n):
    return jnp.where(member % 2 == 0, member // 2, n - 1 - member // 2)


def ring_member(position, n):
    position = lax.rem(position + 2 * n, n)
    return jnp.where(position < n // 2, 2 * position, 2 * (n - 1 - position) + 1)


def swap_pairs(x):
    lane = lax.broadcasted_iota(jnp.int32, x.shape, 1)
    width = x.shape[1]
    return jnp.where(lane % 2 == 0, pltpu.roll(x, width - 1, 1), pltpu.roll(x, 1, 1))


def layer_kernel(
    n, chunks, pieces, arriving, gain_hbm, wq, wk, wv, w_hbm, tables_hbm,
    attended_ref, stream_ref,
    staged, gain, tables, x_all, weights, acc, squares, sent, got, heads_kv, key_head, value_head, q_ref, w_out, context, running,
    stage_sem, gain_sem, tables_sem, w_sem, wo_sem, shift_send, shift_recv, ring_send, ring_recv, kv_send, kv_recv, send_sem, recv_sem,
):
    sections = lax.axis_size("section")
    section = lax.axis_index("section")
    me = lax.axis_index("mp")
    position = ring_position(me, n)
    right, left = ring_member(position + 1, n), ring_member(position - 1, n)
    following, previous = lax.rem(section + 1, sections), lax.rem(section + sections - 1, sections)
    hops = n // 2
    per = n // chunks
    rows, width = x_all.shape[2:]
    length = n * rows
    chunk_rows = per * rows
    qw, kw, vw = wq.shape[0], wk.shape[0], wv.shape[0]
    heads = qw // HD
    group_size = heads * n // KV_HEADS
    nn = (((1,), (0,)), ((), ()))
    nt = (((1,), (1,)), ((), ()))

    stage = pltpu.make_async_copy(arriving, staged, stage_sem)
    stage.start()
    gain_copy = pltpu.make_async_copy(gain_hbm, gain, gain_sem)
    gain_copy.start()
    tables_copy = pltpu.make_async_copy(tables_hbm, tables, tables_sem)
    tables_copy.start()
    barrier = pltpu.get_barrier_semaphore()
    for step in range(1, n):
        pl.semaphore_signal(barrier, inc=1, device_id={"mp": lax.rem(me + step, n)}, device_id_type=MESH)
    for partner in (following, previous):
        pl.semaphore_signal(barrier, inc=1, device_id={"section": partner}, device_id_type=MESH)

    def weight_copy(j, part):
        src, start, size = ((wq, 0, qw), (wk, qw, kw), (wv, qw + kw, vw))[part]
        return pltpu.make_async_copy(
            src.at[:, pl.ds(j * width, width)], weights.at[j, pl.ds(start, size)], w_sem.at[j, part]
        )

    def shift_copy(c):
        return pltpu.make_async_remote_copy(
            src_ref=staged.at[pl.ds(c * per, per)],
            dst_ref=x_all.at[me, pl.ds(c * per, per)],
            send_sem=shift_send.at[c], recv_sem=shift_recv.at[c],
            device_id={"section": following}, device_id_type=MESH,
        )

    def ring_copy(way, hop, c):
        origin = ring_member(position - (hop - 1) if way == 0 else position + (hop - 1), n)
        return pltpu.make_async_remote_copy(
            src_ref=x_all.at[origin, pl.ds(c * per, per)],
            dst_ref=x_all.at[origin, pl.ds(c * per, per)],
            send_sem=ring_send.at[way, hop - 1, c], recv_sem=ring_recv.at[way, hop - 1, c],
            device_id={"mp": right if way == 0 else left}, device_id_type=MESH,
        )

    for j in range(n):
        for part in range(3):
            weight_copy(j, part).start()
    stage.wait()
    pl.semaphore_wait(barrier, n + 1)
    for c in range(chunks):
        shift_copy(c).start()
    acc[...] = jnp.zeros_like(acc)
    squares[...] = jnp.zeros_like(squares)

    def compute(slot, c):
        x = x_all[slot, pl.ds(c * per, per)].astype(jnp.float32).reshape(chunk_rows, width)
        total = x[:, :128] * x[:, :128]
        for g in range(1, width // 128):
            part = x[:, g * 128 : (g + 1) * 128]
            total = total + part * part
        squares[c] += total
        scaled = (x * gain[slot].astype(jnp.float32)).astype(jnp.bfloat16)
        acc[c] += lax.dot_general(scaled, weights[slot], nt, preferred_element_type=jnp.float32)

    for c in range(chunks):
        shift_copy(c).wait_recv()
        ring_copy(0, 1, c).start()
        ring_copy(1, 1, c).start()
    for j in range(n):
        for part in range(3):
            weight_copy(j, part).wait()
    gain_copy.wait()
    tables_copy.wait()
    wo_copy = pltpu.make_async_copy(w_hbm, w_out, wo_sem)
    wo_copy.start()

    @pl.loop(0, chunks)
    def _(c):
        compute(me, c)

    cos, sin = tables[0], tables[1]
    lane = lax.broadcasted_iota(jnp.int32, (HD, kw), 1)
    source = lax.broadcasted_iota(jnp.int32, (HD, kw), 0)
    pick = (source == (me * kw + lane) // (2 * KV_HEADS) * 2 + lane % 2).astype(jnp.float32)
    k_cos = lax.dot_general(cos, pick, nn, precision=lax.Precision.HIGHEST, preferred_element_type=jnp.float32)
    k_sin = lax.dot_general(sin, pick, nn, precision=lax.Precision.HIGHEST, preferred_element_type=jnp.float32)
    per_head = kw // KV_HEADS
    target = lax.broadcasted_iota(jnp.int32, (kw, kw), 0)
    origin_row = lax.broadcasted_iota(jnp.int32, (kw, kw), 1)
    head, within = target // per_head, target % per_head
    order = (origin_row == (within // 2 * KV_HEADS + head) * 2 + within % 2).astype(jnp.bfloat16)

    @pl.loop(0, hops * chunks)
    def _(i):
        hop = i // chunks + 1
        turn = lax.rem(i, chunks)
        last = hop == hops
        c = jnp.where(last, turn // 2 + lax.rem(turn, 2) * (chunks // 2), turn)
        low = c < chunks // 2
        for way in range(2):
            mine = low if way == 0 else jnp.logical_not(low)

            @pl.when(jnp.logical_or(jnp.logical_not(last), mine))
            def _():
                ring_copy(way, hop, c).wait_recv()

            @pl.when(jnp.logical_and(hop < hops, jnp.logical_or(hop + 1 < hops, mine)))
            def _():
                ring_copy(way, hop + 1, c).start()

        @pl.loop(0, 2)
        def _(way):
            mine = low == (way == 0)

            @pl.when(jnp.logical_or(jnp.logical_not(last), mine))
            def _():
                compute(ring_member(jnp.where(way == 0, position - hop, position + hop), n), c)

    inverse = lax.rsqrt(
        jnp.sum(squares[...].reshape(length, 128), axis=1, keepdims=True) * (1.0 / (n * width)) + NORM_EPS
    )
    k = acc[:, :, qw : qw + kw].reshape(length, kw) * inverse
    k_rot = (k * k_cos + swap_pairs(k) * k_sin).astype(jnp.bfloat16)
    v_bf = (acc[:, :, qw + kw :].reshape(length, vw) * inverse).astype(jnp.bfloat16)
    for part, rotated in enumerate((k_rot, v_bf)):
        ordered = lax.dot_general(order, rotated, nt, preferred_element_type=jnp.float32)
        for h in range(KV_HEADS):
            sent[h, part] = ordered[h * per_head : (h + 1) * per_head].astype(jnp.bfloat16)

    def kv_copy(part, step):
        other = lax.rem(me + step, n)
        return pltpu.make_async_remote_copy(
            src_ref=sent.at[other * heads // group_size, part], dst_ref=got.at[me, part],
            send_sem=kv_send.at[part, step - 1], recv_sem=kv_recv.at[part, step - 1],
            device_id={"mp": other}, device_id_type=MESH,
        )

    for part in range(2):
        for step in range(1, n):
            kv_copy(part, step).start()
    got[me] = sent[me * heads // group_size]
    for h in range(heads):
        q = acc[:, :, h * HD : (h + 1) * HD].reshape(length, HD) * inverse
        q_ref[:, :, h * HD : (h + 1) * HD] = (
            (q * cos + swap_pairs(q) * sin).reshape(n, rows, HD).astype(jnp.bfloat16)
        )

    def receive(part, whole):
        for step in range(1, n):
            kv_copy(part, step).wait_recv()
        for j in range(n):
            heads_kv[part, j * per_head : (j + 1) * per_head] = got[j, part].astype(jnp.float32)
        whole[...] = heads_kv[part].astype(jnp.bfloat16)

    receive(0, key_head)

    piece_width = running.shape[4]
    scale = 1.0 / math.sqrt(HD)

    def attend(block, ready=None):
        row = lax.broadcasted_iota(jnp.int32, (rows, length), 0) + block * rows
        column = lax.broadcasted_iota(jnp.int32, (rows, length), 1)
        probs = []
        for h in range(heads):
            q = q_ref[block, :, h * HD : (h + 1) * HD]
            scores = lax.dot_general(q, key_head[...], nn, preferred_element_type=jnp.float32) * scale
            scores = jnp.where(row >= column, scores, -1e30)
            exponent = jnp.exp(scores - jnp.max(scores, axis=1, keepdims=True))
            probs.append((exponent / jnp.sum(exponent, axis=1, keepdims=True)).astype(jnp.bfloat16))
        if ready is not None:
            ready()
        for h in range(heads):
            context[block, :, h * HD : (h + 1) * HD] = lax.dot_general(
                probs[h], value_head[...], nt, preferred_element_type=jnp.float32
            ).astype(jnp.bfloat16)

    def block_of(way, step):
        return ring_member(position - 1 - step if way == 0 else position + 1 + step, n)

    def term(way, step, piece):
        start = (way * pieces + piece) * piece_width
        return jnp.dot(
            context[block_of(way, step)], w_out[:, start : start + piece_width], preferred_element_type=jnp.float32
        )

    def sum_copy(way, step, piece):
        return pltpu.make_async_remote_copy(
            src_ref=running.at[way, step, piece],
            dst_ref=running.at[way, step + 1, piece],
            send_sem=send_sem.at[way, step, piece], recv_sem=recv_sem.at[way, step, piece],
            device_id={"mp": right if way == 0 else left}, device_id_type=MESH,
        )

    wo_copy.wait()
    for way in range(2):
        attend(block_of(way, 0), functools.partial(receive, 1, value_head) if way == 0 else None)
        for piece in range(pieces):
            running[way, 0, piece] = term(way, 0, piece).astype(jnp.bfloat16)
            sum_copy(way, 0, piece).start()

    def ahead(step):
        @pl.when(step < n // 2)
        def _():
            attend(block_of(0, step))
            attend(block_of(1, step))

        @pl.when(step == n // 2)
        def _():
            attend(me)

    ahead(1)

    @pl.loop(1, n - 1)
    def _(step):
        for piece in range(pieces):
            for way in range(2):
                value = term(way, step, piece)
                sum_copy(way, step - 1, piece).wait_recv()
                running[way, step, piece] = (running[way, step, piece].astype(jnp.float32) + value).astype(jnp.bfloat16)
                sum_copy(way, step, piece).start()
        ahead(step + 1)

    for j in range(n):
        stream_ref[:, j * width : (j + 1) * width] = x_all[j, me]
    for piece in range(pieces):
        for way in range(2):
            value = term(way, n - 1, piece)
            sum_copy(way, n - 2, piece).wait_recv()
            value = running[way, n - 1, piece].astype(jnp.float32) + value
            columns = slice((way * pieces + piece) * piece_width, (way * pieces + piece + 1) * piece_width)
            attended_ref[:, columns] = value.astype(jnp.bfloat16)
            stream_ref[:, columns] = (stream_ref[:, columns].astype(jnp.float32) + value).astype(jnp.bfloat16)

    for c in range(chunks):
        shift_copy(c).wait_send()
    for part in range(2):
        for step in range(1, n):
            kv_copy(part, step).wait_send()

    @pl.loop(0, hops * chunks)
    def _(i):
        hop = i // chunks + 1
        c = lax.rem(i, chunks)
        for way in range(2):
            mine = (c < chunks // 2) if way == 0 else (c >= chunks // 2)

            @pl.when(jnp.logical_or(hop < hops, mine))
            def _():
                ring_copy(way, hop, c).wait_send()

    @pl.loop(0, n - 1)
    def _(step):
        for piece in range(pieces):
            for way in range(2):
                sum_copy(way, step, piece).wait_send()


def rotary_tables(length):
    pair = (np.arange(HD) // 2).astype(np.float32)
    frequency = np.exp(pair * np.float32(-2.0 * math.log(ROPE_BASE) / HD)).astype(np.float32)
    angles = frequency[None, :] * np.arange(length, dtype=np.float32)[:, None]
    sign = np.where(np.arange(HD) % 2 == 0, -1.0, 1.0).astype(np.float32)
    return np.stack([np.cos(angles), np.sin(angles) * sign]).astype(np.float32)


def local(arriving, norm_gain, w_query, w_key, w_value, w_out):
    n = lax.axis_size("mp")
    length, width = arriving.shape[1:]
    rows = length // n
    full = n * width
    chunks = 8 if n <= 8 else 2
    pieces = 4 if n <= 8 else 2
    qw, kw, vw = w_query.shape[1], w_key.shape[1], w_value.shape[1]
    tables = rotary_tables(length)
    vmem = pl.BlockSpec(memory_space=pltpu.VMEM)
    hbm = pl.BlockSpec(memory_space=pltpu.HBM)
    bf16, f32 = jnp.bfloat16, jnp.float32
    dma = pltpu.SemaphoreType.DMA
    attended, stream = pl.pallas_call(
        functools.partial(layer_kernel, n, chunks, pieces),
        name="layer",
        out_shape=(pltpu.VMEM((rows, full), bf16),) * 2,
        in_specs=[hbm] * 7,
        out_specs=(vmem, vmem),
        scratch_shapes=[
            pltpu.VMEM((n, rows, width), bf16),
            pltpu.VMEM((n, 1, width), bf16),
            pltpu.VMEM((2, length, HD), f32),
            pltpu.VMEM((n, n, rows, width), bf16),
            pltpu.VMEM((n, qw + kw + vw, width), bf16),
            pltpu.VMEM((chunks, length // chunks, qw + kw + vw), f32),
            pltpu.VMEM((chunks, length // chunks, 128), f32),
            pltpu.VMEM((KV_HEADS, 2, kw // KV_HEADS, length), bf16),
            pltpu.VMEM((n, 2, kw // KV_HEADS, length), bf16),
            pltpu.VMEM((2, HD, length), f32),
            pltpu.VMEM((HD, length), bf16),
            pltpu.VMEM((HD, length), bf16),
            pltpu.VMEM((n, rows, qw), bf16),
            pltpu.VMEM((qw, full), bf16),
            pltpu.VMEM((n, rows, qw), bf16),
            pltpu.VMEM((2, n, pieces, rows, full // (2 * pieces)), bf16),
            dma(()),
            dma(()),
            dma(()),
            dma((n, 3)),
            dma(()),
            dma((chunks,)),
            dma((chunks,)),
            dma((2, n // 2, chunks)),
            dma((2, n // 2, chunks)),
            dma((2, n - 1)),
            dma((2, n - 1)),
            dma((2, n - 1, pieces)),
            dma((2, n - 1, pieces)),
        ],
        compiler_params=pltpu.CompilerParams(collective_id=0, has_side_effects=True, vmem_limit_bytes=VMEM_LIMIT),
    )(
        arriving[0].reshape(n, rows, width),
        norm_gain[0].reshape(n, 1, width),
        w_query[0], w_key[0], w_value[0], w_out[0], jnp.asarray(tables),
    )
    return (attended[None], stream[None])


def solution(mesh):
    return jax.shard_map(
        local,
        mesh=mesh,
        in_specs=(
            P("section", None, "mp"),
            P("section", None),
            P("section", "mp", None),
            P("section", "mp", None),
            P("section", "mp", None),
            P("section", "mp", None),
        ),
        out_specs=(P("section", "mp", None), P("section", "mp", None)),
        check_vma=False,
    )
```

```python
import functools
import math

import jax
import jax.numpy as jnp
import numpy as np
from jax import lax
from jax.experimental import pallas as pl
from jax.experimental.pallas import tpu as pltpu
from jax.sharding import PartitionSpec as P

HD = 128
KV_HEADS = 8
ROPE_BASE = 500000.0
NORM_EPS = 1e-05
MESH = pl.DeviceIdType.MESH
VMEM_LIMIT = 63500000


def ring_position(member, n):
    return jnp.where(member % 2 == 0, member // 2, n - 1 - member // 2)


def ring_member(position, n):
    position = lax.rem(position + 2 * n, n)
    return jnp.where(position < n // 2, 2 * position, 2 * (n - 1 - position) + 1)


def swap_pairs(x):
    lane = lax.broadcasted_iota(jnp.int32, x.shape, 1)
    width = x.shape[1]
    return jnp.where(lane % 2 == 0, pltpu.roll(x, width - 1, 1), pltpu.roll(x, 1, 1))


def layer_kernel(
    n, chunks, pieces, arriving, gain_hbm, wq, wk, wv, w_hbm, tables_hbm,
    attended_ref, stream_ref,
    staged, gain, tables, x_all, weights, acc, squares, sent, got, heads_kv, key_head, value_head, q_ref, w_out, context, running,
    stage_sem, gain_sem, tables_sem, w_sem, wo_sem, shift_send, shift_recv, ring_send, ring_recv, kv_send, kv_recv, send_sem, recv_sem,
):
    sections = lax.axis_size("section")
    section = lax.axis_index("section")
    me = lax.axis_index("mp")
    position = ring_position(me, n)
    right, left = ring_member(position + 1, n), ring_member(position - 1, n)
    following, previous = lax.rem(section + 1, sections), lax.rem(section + sections - 1, sections)
    hops = n // 2
    per = n // chunks
    rows, width = x_all.shape[2:]
    length = n * rows
    chunk_rows = per * rows
    qw, kw, vw = wq.shape[0], wk.shape[0], wv.shape[0]
    heads = qw // HD
    group_size = heads * n // KV_HEADS
    nn = (((1,), (0,)), ((), ()))
    nt = (((1,), (1,)), ((), ()))

    stage = pltpu.make_async_copy(arriving, staged, stage_sem)
    stage.start()
    gain_copy = pltpu.make_async_copy(gain_hbm, gain, gain_sem)
    gain_copy.start()
    tables_copy = pltpu.make_async_copy(tables_hbm, tables, tables_sem)
    tables_copy.start()
    barrier = pltpu.get_barrier_semaphore()
    for step in range(1, n):
        pl.semaphore_signal(barrier, inc=1, device_id={"mp": lax.rem(me + step, n)}, device_id_type=MESH)
    for partner in (following, previous):
        pl.semaphore_signal(barrier, inc=1, device_id={"section": partner}, device_id_type=MESH)

    def weight_copy(j, part):
        src, start, size = ((wq, 0, qw), (wk, qw, kw), (wv, qw + kw, vw))[part]
        return pltpu.make_async_copy(
            src.at[:, pl.ds(j * width, width)], weights.at[j, pl.ds(start, size)], w_sem.at[j, part]
        )

    def shift_copy(c):
        return pltpu.make_async_remote_copy(
            src_ref=staged.at[pl.ds(c * per, per)],
            dst_ref=x_all.at[me, pl.ds(c * per, per)],
            send_sem=shift_send.at[c], recv_sem=shift_recv.at[c],
            device_id={"section": following}, device_id_type=MESH,
        )

    def ring_copy(way, hop, c):
        origin = ring_member(position - (hop - 1) if way == 0 else position + (hop - 1), n)
        return pltpu.make_async_remote_copy(
            src_ref=x_all.at[origin, pl.ds(c * per, per)],
            dst_ref=x_all.at[origin, pl.ds(c * per, per)],
            send_sem=ring_send.at[way, hop - 1, c], recv_sem=ring_recv.at[way, hop - 1, c],
            device_id={"mp": right if way == 0 else left}, device_id_type=MESH,
        )

    for j in range(n):
        for part in range(3):
            weight_copy(j, part).start()
    stage.wait()
    pl.semaphore_wait(barrier, n + 1)
    for c in range(chunks):
        shift_copy(c).start()
    acc[...] = jnp.zeros_like(acc)
    squares[...] = jnp.zeros_like(squares)

    def compute(slot, c):
        x = x_all[slot, pl.ds(c * per, per)].astype(jnp.float32).reshape(chunk_rows, width)
        total = x[:, :128] * x[:, :128]
        for g in range(1, width // 128):
            part = x[:, g * 128 : (g + 1) * 128]
            total = total + part * part
        squares[c] += total
        scaled = (x * gain[slot].astype(jnp.float32)).astype(jnp.bfloat16)
        acc[c] += lax.dot_general(scaled, weights[slot], nt, preferred_element_type=jnp.float32)

    for c in range(chunks):
        shift_copy(c).wait_recv()
        ring_copy(0, 1, c).start()
        ring_copy(1, 1, c).start()
    for j in range(n):
        for part in range(3):
            weight_copy(j, part).wait()
    gain_copy.wait()
    tables_copy.wait()
    wo_copy = pltpu.make_async_copy(w_hbm, w_out, wo_sem)
    wo_copy.start()

    @pl.loop(0, chunks)
    def _(c):
        compute(me, c)

    cos, sin = tables[0], tables[1]
    lane = lax.broadcasted_iota(jnp.int32, (HD, kw), 1)
    source = lax.broadcasted_iota(jnp.int32, (HD, kw), 0)
    pick = (source == (me * kw + lane) // (2 * KV_HEADS) * 2 + lane % 2).astype(jnp.float32)
    k_cos = lax.dot_general(cos, pick, nn, precision=lax.Precision.HIGHEST, preferred_element_type=jnp.float32)
    k_sin = lax.dot_general(sin, pick, nn, precision=lax.Precision.HIGHEST, preferred_element_type=jnp.float32)
    per_head = kw // KV_HEADS
    target = lax.broadcasted_iota(jnp.int32, (kw, kw), 0)
    origin_row = lax.broadcasted_iota(jnp.int32, (kw, kw), 1)
    head, within = target // per_head, target % per_head
    order = (origin_row == (within // 2 * KV_HEADS + head) * 2 + within % 2).astype(jnp.bfloat16)

    @pl.loop(0, hops * chunks)
    def _(i):
        hop = i // chunks + 1
        turn = lax.rem(i, chunks)
        last = hop == hops
        c = jnp.where(last, turn // 2 + lax.rem(turn, 2) * (chunks // 2), turn)
        low = c < chunks // 2
        for way in range(2):
            mine = low if way == 0 else jnp.logical_not(low)

            @pl.when(jnp.logical_or(jnp.logical_not(last), mine))
            def _():
                ring_copy(way, hop, c).wait_recv()

            @pl.when(jnp.logical_and(hop < hops, jnp.logical_or(hop + 1 < hops, mine)))
            def _():
                ring_copy(way, hop + 1, c).start()

        @pl.loop(0, 2)
        def _(way):
            mine = low == (way == 0)

            @pl.when(jnp.logical_or(jnp.logical_not(last), mine))
            def _():
                compute(ring_member(jnp.where(way == 0, position - hop, position + hop), n), c)

    inverse = lax.rsqrt(
        jnp.sum(squares[...].reshape(length, 128), axis=1, keepdims=True) * (1.0 / (n * width)) + NORM_EPS
    )
    k = acc[:, :, qw : qw + kw].reshape(length, kw) * inverse
    k_rot = (k * k_cos + swap_pairs(k) * k_sin).astype(jnp.bfloat16)
    def kv_copy(part, step):
        other = lax.rem(me + step, n)
        return pltpu.make_async_remote_copy(
            src_ref=sent.at[other * heads // group_size, part], dst_ref=got.at[me, part],
            send_sem=kv_send.at[part, step - 1], recv_sem=kv_recv.at[part, step - 1],
            device_id={"mp": other}, device_id_type=MESH,
        )

    def order_and_send(part, channels):
        ordered = lax.dot_general(order, channels, nt, preferred_element_type=jnp.float32)
        for h in range(KV_HEADS):
            sent[h, part] = ordered[h * per_head : (h + 1) * per_head].astype(jnp.bfloat16)
        for step in range(1, n):
            kv_copy(part, step).start()

    order_and_send(0, k_rot)
    order_and_send(1, (acc[:, :, qw + kw :].reshape(length, vw) * inverse).astype(jnp.bfloat16))
    got[me] = sent[me * heads // group_size]
    for h in range(heads):
        q = acc[:, :, h * HD : (h + 1) * HD].reshape(length, HD) * inverse
        q_ref[:, :, h * HD : (h + 1) * HD] = (
            (q * cos + swap_pairs(q) * sin).reshape(n, rows, HD).astype(jnp.bfloat16)
        )

    def receive(part, whole):
        for step in range(1, n):
            kv_copy(part, step).wait_recv()
        for j in range(n):
            heads_kv[part, j * per_head : (j + 1) * per_head] = got[j, part].astype(jnp.float32)
        whole[...] = heads_kv[part].astype(jnp.bfloat16)

    receive(0, key_head)

    piece_width = running.shape[4]
    scale = 1.0 / math.sqrt(HD)

    def attend(block, ready=None):
        row = lax.broadcasted_iota(jnp.int32, (rows, length), 0) + block * rows
        column = lax.broadcasted_iota(jnp.int32, (rows, length), 1)
        probs = []
        for h in range(heads):
            q = q_ref[block, :, h * HD : (h + 1) * HD]
            scores = lax.dot_general(q, key_head[...], nn, preferred_element_type=jnp.float32) * scale
            scores = jnp.where(row >= column, scores, -1e30)
            exponent = jnp.exp(scores - jnp.max(scores, axis=1, keepdims=True))
            probs.append((exponent / jnp.sum(exponent, axis=1, keepdims=True)).astype(jnp.bfloat16))
        if ready is not None:
            ready()
        for h in range(heads):
            context[block, :, h * HD : (h + 1) * HD] = lax.dot_general(
                probs[h], value_head[...], nt, preferred_element_type=jnp.float32
            ).astype(jnp.bfloat16)

    def block_of(way, step):
        return ring_member(position - 1 - step if way == 0 else position + 1 + step, n)

    def term(way, step, piece):
        start = (way * pieces + piece) * piece_width
        return jnp.dot(
            context[block_of(way, step)], w_out[:, start : start + piece_width], preferred_element_type=jnp.float32
        )

    def sum_copy(way, step, piece):
        return pltpu.make_async_remote_copy(
            src_ref=running.at[way, step, piece],
            dst_ref=running.at[way, step + 1, piece],
            send_sem=send_sem.at[way, step, piece], recv_sem=recv_sem.at[way, step, piece],
            device_id={"mp": right if way == 0 else left}, device_id_type=MESH,
        )

    wo_copy.wait()
    for way in range(2):
        attend(block_of(way, 0), functools.partial(receive, 1, value_head) if way == 0 else None)
        for piece in range(pieces):
            running[way, 0, piece] = term(way, 0, piece).astype(jnp.bfloat16)
            sum_copy(way, 0, piece).start()

    def ahead(step):
        @pl.when(step < n // 2)
        def _():
            attend(block_of(0, step))
            attend(block_of(1, step))

        @pl.when(step == n // 2)
        def _():
            attend(me)

    ahead(1)

    @pl.loop(1, n - 1)
    def _(step):
        for piece in range(pieces):
            for way in range(2):
                value = term(way, step, piece)
                sum_copy(way, step - 1, piece).wait_recv()
                running[way, step, piece] = (running[way, step, piece].astype(jnp.float32) + value).astype(jnp.bfloat16)
                sum_copy(way, step, piece).start()
        ahead(step + 1)

    for j in range(n):
        stream_ref[:, j * width : (j + 1) * width] = x_all[j, me]
    for piece in range(pieces):
        for way in range(2):
            value = term(way, n - 1, piece)
            sum_copy(way, n - 2, piece).wait_recv()
            value = running[way, n - 1, piece].astype(jnp.float32) + value
            columns = slice((way * pieces + piece) * piece_width, (way * pieces + piece + 1) * piece_width)
            attended_ref[:, columns] = value.astype(jnp.bfloat16)
            stream_ref[:, columns] = (stream_ref[:, columns].astype(jnp.float32) + value).astype(jnp.bfloat16)

    for c in range(chunks):
        shift_copy(c).wait_send()
    for part in range(2):
        for step in range(1, n):
            kv_copy(part, step).wait_send()

    @pl.loop(0, hops * chunks)
    def _(i):
        hop = i // chunks + 1
        c = lax.rem(i, chunks)
        for way in range(2):
            mine = (c < chunks // 2) if way == 0 else (c >= chunks // 2)

            @pl.when(jnp.logical_or(hop < hops, mine))
            def _():
                ring_copy(way, hop, c).wait_send()

    @pl.loop(0, n - 1)
    def _(step):
        for piece in range(pieces):
            for way in range(2):
                sum_copy(way, step, piece).wait_send()


def rotary_tables(length):
    pair = (np.arange(HD) // 2).astype(np.float32)
    frequency = np.exp(pair * np.float32(-2.0 * math.log(ROPE_BASE) / HD)).astype(np.float32)
    angles = frequency[None, :] * np.arange(length, dtype=np.float32)[:, None]
    sign = np.where(np.arange(HD) % 2 == 0, -1.0, 1.0).astype(np.float32)
    return np.stack([np.cos(angles), np.sin(angles) * sign]).astype(np.float32)


def local(arriving, norm_gain, w_query, w_key, w_value, w_out):
    n = lax.axis_size("mp")
    length, width = arriving.shape[1:]
    rows = length // n
    full = n * width
    chunks = 8 if n <= 8 else 2
    pieces = 4 if n <= 8 else 2
    qw, kw, vw = w_query.shape[1], w_key.shape[1], w_value.shape[1]
    tables = rotary_tables(length)
    vmem = pl.BlockSpec(memory_space=pltpu.VMEM)
    hbm = pl.BlockSpec(memory_space=pltpu.HBM)
    bf16, f32 = jnp.bfloat16, jnp.float32
    dma = pltpu.SemaphoreType.DMA
    attended, stream = pl.pallas_call(
        functools.partial(layer_kernel, n, chunks, pieces),
        name="layer",
        out_shape=(pltpu.VMEM((rows, full), bf16),) * 2,
        in_specs=[hbm] * 7,
        out_specs=(vmem, vmem),
        scratch_shapes=[
            pltpu.VMEM((n, rows, width), bf16),
            pltpu.VMEM((n, 1, width), bf16),
            pltpu.VMEM((2, length, HD), f32),
            pltpu.VMEM((n, n, rows, width), bf16),
            pltpu.VMEM((n, qw + kw + vw, width), bf16),
            pltpu.VMEM((chunks, length // chunks, qw + kw + vw), f32),
            pltpu.VMEM((chunks, length // chunks, 128), f32),
            pltpu.VMEM((KV_HEADS, 2, kw // KV_HEADS, length), bf16),
            pltpu.VMEM((n, 2, kw // KV_HEADS, length), bf16),
            pltpu.VMEM((2, HD, length), f32),
            pltpu.VMEM((HD, length), bf16),
            pltpu.VMEM((HD, length), bf16),
            pltpu.VMEM((n, rows, qw), bf16),
            pltpu.VMEM((qw, full), bf16),
            pltpu.VMEM((n, rows, qw), bf16),
            pltpu.VMEM((2, n, pieces, rows, full // (2 * pieces)), bf16),
            dma(()),
            dma(()),
            dma(()),
            dma((n, 3)),
            dma(()),
            dma((chunks,)),
            dma((chunks,)),
            dma((2, n // 2, chunks)),
            dma((2, n // 2, chunks)),
            dma((2, n - 1)),
            dma((2, n - 1)),
            dma((2, n - 1, pieces)),
            dma((2, n - 1, pieces)),
        ],
        compiler_params=pltpu.CompilerParams(collective_id=0, has_side_effects=True, vmem_limit_bytes=VMEM_LIMIT),
    )(
        arriving[0].reshape(n, rows, width),
        norm_gain[0].reshape(n, 1, width),
        w_query[0], w_key[0], w_value[0], w_out[0], jnp.asarray(tables),
    )
    return (attended[None], stream[None])


def solution(mesh):
    return jax.shard_map(
        local,
        mesh=mesh,
        in_specs=(
            P("section", None, "mp"),
            P("section", None),
            P("section", "mp", None),
            P("section", "mp", None),
            P("section", "mp", None),
            P("section", "mp", None),
        ),
        out_specs=(P("section", "mp", None), P("section", "mp", None)),
        check_vma=False,
    )
```
